32 devices in a mesh: rows: 8 (over z, y), rank: 4 (over x, core).
Axes of the slice: x: 2, y: 2, z: 4, core: 2. Of those that a mesh axis runs over, the one named last changes fastest.
Arguments:
- left_factor: bfloat16 [128, 16384], P(None, 'rows'), may hold values from -8 to 8
- right_factor: bfloat16 [128, 16384], P(None, 'rows'), may hold values from -8 to 8
- left_plan: float32 [256, 16384], P('rank', 'rows'), may hold values from 0.0068 to 147, as said below
- right_plan: float32 [256, 16384], P('rank', 'rows'), may hold values from 0.0068 to 147, as said below
- log_inner: float32 [256], P('rank'), may hold values from -1 to 1
- left_mass: float32 [16384], P('rows'), may hold values from 32 to 1024, as said below
- right_mass: float32 [16384], P('rows'), may hold values from 32 to 1024, as said below
Outputs:
- new_left: float32 [256, 16384], P('rank', 'rows')
- new_right: float32 [256, 16384], P('rank', 'rows')
- new_log_inner: float32 [256], P('rank')
The draws below stay inside these ranges and needn't reach their ends.
Inputs may be any that keep to these rules, and one draw needn't show every extreme that they name: `left_plan`: positive entries. `right_plan`: positive entries. `left_mass`: positive point masses. `right_mass`: positive point masses.
All inputs are finite; a program needn't handle non-finite values. Where the reference program divides by a largest or mean magnitude, that divisor is 1e-20 or more.
Results may differ from the reference program's by a relative error of at most 0.00045.
Values sent between devices are 32-bit elements; how exact they have to be, the bound alone decides.
No kernel may reach another device: no remote copies, remote signals or barrier semaphores. Data moves between devices by JAX's collectives and lax.ppermute only.
A program may use at most 64 MiB of HBM per device.

```python
import math
import jax
import jax.numpy as jnp
from jax import lax

DC = 128
RANK = 256
ROWS_DEV = 2048
ITERS = 3
POINTS = 16384


def draw_masses(key):
    blocks = POINTS // ROWS_DEV
    level = jnp.exp(jax.random.uniform(jax.random.fold_in(key, 1), (blocks, 1), jnp.float32, math.log(32.0), math.log(512.0)))
    factor = jax.random.uniform(jax.random.fold_in(key, 2), (blocks, ROWS_DEV), jnp.float32, 1.0, 2.0)
    return (level * factor).reshape(POINTS)


def draw_left_mass(key, part):
    return draw_masses(jax.random.fold_in(key, 11))


def draw_right_mass(key, part):
    return draw_masses(jax.random.fold_in(key, 23))


def draw_points(key, salt):
    blocks = POINTS // ROWS_DEV
    inner_key = jax.random.fold_in(key, salt)
    offset = jax.random.uniform(jax.random.fold_in(inner_key, 5), (blocks, 1), jnp.float32, -1.25, 1.25)
    offset = jnp.broadcast_to(offset, (blocks, ROWS_DEV)).reshape(1, POINTS)
    noise = jax.random.truncated_normal(jax.random.fold_in(inner_key, 2), -2.75, 2.75, (DC, POINTS), jnp.float32)
    return jnp.clip(noise + offset, -4.0, 4.0)


def draw_directions(key):
    return jax.random.normal(jax.random.fold_in(key, 307), (DC, RANK), jnp.float32) / math.sqrt(DC)


def draw_plan(key, salt):
    blocks = POINTS // ROWS_DEV
    inner_key = jax.random.fold_in(key, salt)
    points = draw_points(key, salt)
    directions = draw_directions(key)
    align = jnp.dot(directions.T, points, precision=lax.Precision.HIGHEST)
    align = jnp.clip(align, -3.0, 3.0).reshape(RANK, blocks, ROWS_DEV)
    strength = jax.random.uniform(jax.random.fold_in(inner_key, 3), (1, blocks, 1), jnp.float32, 0.4, 1.2)
    leaning = jnp.exp(strength * align).reshape(RANK, POINTS)
    base = jnp.exp(jax.random.uniform(jax.random.fold_in(inner_key, 4), (RANK, POINTS), jnp.float32, math.log(0.25), math.log(4.0)))
    return base * leaning


def draw_left_factor(key, part):
    return (2.0 * draw_points(key, 101)).astype(jnp.bfloat16)


def draw_right_factor(key, part):
    return (2.0 * draw_points(key, 202)).astype(jnp.bfloat16)


def draw_left_plan(key, part):
    return draw_plan(key, 101)


def draw_right_plan(key, part):
    return draw_plan(key, 202)


def shard_levels(key, extent, split, low, top_value):
    def one(position, parts):
        heights = jax.random.uniform(jax.random.fold_in(jax.random.fold_in(key, 6), position), (parts,), jnp.float32, low / len(split), top_value / len(split))
        return jnp.repeat(jnp.exp(heights), extent[position] // parts).reshape((-1,) + (1,) * (len(extent) - position - 1))

    loudness = one(*split[0])
    for cut in split[1:]:
        loudness = loudness * one(*cut)
    return loudness


def setup_inputs(seed: int = 0) -> dict:
    keys = jax.random.split(jax.random.key(seed), 8)
    left_factor = draw_left_factor(jax.random.fold_in(keys[7], 71), 0)
    right_factor = draw_right_factor(jax.random.fold_in(keys[7], 71), 0)
    left_plan = draw_left_plan(jax.random.fold_in(keys[7], 71), 0)
    right_plan = draw_right_plan(jax.random.fold_in(keys[7], 71), 0)
    log_inner = jnp.clip(jax.random.uniform(keys[4], (RANK,), jnp.float32, -1.0, 1.0) * shard_levels(keys[4], (RANK,), ((0, 4),), -0.4, 0.0), -1.0, 1.0)
    left_mass = draw_left_mass(jax.random.fold_in(keys[7], 71), 0)
    right_mass = draw_right_mass(jax.random.fold_in(keys[7], 71), 0)
    return {"left_factor": left_factor, "right_factor": right_factor, "left_plan": left_plan, "right_plan": right_plan, "log_inner": log_inner, "left_mass": left_mass, "right_mass": right_mass}


def balance(inner_mass, col_scale_left, col_total_left, col_scale_right, col_total_right):
    mixed = jnp.log(inner_mass) + jnp.log(col_scale_left * col_total_left) + jnp.log(col_scale_right * col_total_right)
    inner_mass = jnp.exp(mixed / 3.0)
    return inner_mass, inner_mass / col_total_left, inner_mass / col_total_right


def reference(left_factor, right_factor, left_plan, right_plan, log_inner, left_mass, right_mass):
    precise = lax.Precision.HIGHEST
    total_left = jnp.sum(left_mass)
    total_right = jnp.sum(right_mass)
    inner_mass = (total_left / RANK) * jnp.exp(log_inner)
    left_round = left_plan.astype(jnp.bfloat16)
    right_round = right_plan.astype(jnp.bfloat16)
    proj_right = jnp.dot(right_factor, right_round.T, preferred_element_type=jnp.float32)
    proj_left = jnp.dot(left_factor, left_round.T, preferred_element_type=jnp.float32)
    scaled_right = (proj_right / inner_mass[None, :]).astype(jnp.bfloat16)
    scaled_left = (proj_left / inner_mass[None, :]).astype(jnp.bfloat16)
    grad_left = jnp.dot(scaled_right.T, left_factor, preferred_element_type=jnp.float32)
    grad_right = jnp.dot(scaled_left.T, right_factor, preferred_element_type=jnp.float32)
    pairing = jnp.sum(left_round.astype(jnp.float32) * grad_left, axis=1)
    grad_inner = -pairing / inner_mass
    largest = jnp.maximum(jnp.maximum(jnp.max(jnp.abs(grad_left)), jnp.max(jnp.abs(grad_right))), jnp.max(jnp.abs(grad_inner)))
    step_size = 5.0 / jnp.maximum(largest, 0.25)
    tilted_left = left_plan * jnp.exp(-step_size * grad_left)
    tilted_right = right_plan * jnp.exp(-step_size * grad_right)
    inner_mass = inner_mass * jnp.exp(-step_size * grad_inner)
    right_norm = right_mass * (total_left / total_right)
    col_scale_left = jnp.ones((RANK,), jnp.float32)
    col_scale_right = jnp.ones((RANK,), jnp.float32)
    row_scale_left = left_mass
    row_scale_right = right_norm
    for repeat in range(ITERS):
        row_scale_left = left_mass / jnp.dot(col_scale_left, tilted_left, precision=precise)
        row_scale_right = right_norm / jnp.dot(col_scale_right, tilted_right, precision=precise)
        col_total_left = jnp.dot(tilted_left, row_scale_left, precision=precise)
        col_total_right = jnp.dot(tilted_right, row_scale_right, precision=precise)
        inner_mass, col_scale_left, col_scale_right = balance(inner_mass, col_scale_left, col_total_left, col_scale_right, col_total_right)
    new_left = row_scale_left[None, :] * tilted_left * col_scale_left[:, None]
    new_right = row_scale_right[None, :] * tilted_right * col_scale_right[:, None]
    new_log_inner = jnp.log(inner_mass) - jnp.log(total_left / RANK)
    return new_left, new_right, new_log_inner
```

```python
import jax
import jax.numpy as jnp
from jax import lax
from jax.sharding import PartitionSpec as P

RANK = 256
ITERS = 3


def contract_points(factor, plan):
    return lax.dot_general(
        factor, plan, (((1,), (1,)), ((), ())), preferred_element_type=jnp.float32
    )


def expand_points(projected, factor):
    return lax.dot_general(
        projected, factor, (((0,), (0,)), ((), ())), preferred_element_type=jnp.float32
    )


def balance(inner_mass, col_scale_left, col_total_left, col_scale_right, col_total_right):
    mixed = (
        jnp.log(inner_mass)
        + jnp.log(col_scale_left * col_total_left)
        + jnp.log(col_scale_right * col_total_right)
    )
    inner_mass = jnp.exp(mixed / 3.0)
    return (inner_mass, inner_mass / col_total_left, inner_mass / col_total_right)


def solution(mesh):
    n_rows = mesh.shape["rows"]
    n_rank = mesh.shape["rank"]
    everyone = ("rows", "rank")
    n_all = n_rows * n_rank

    def sum_over_rows(value):
        if n_rows & (n_rows - 1):
            return lax.psum(value, "rows")
        stride = 1
        while stride < n_rows:
            pairs = [(i, i ^ stride) for i in range(n_rows)]
            value = value + lax.ppermute(value, "rows", pairs)
            stride *= 2
        return value

    def sum_over_rank(value):
        total = value
        for shift in range(1, n_rank):
            pairs = [(i, (i + shift) % n_rank) for i in range(n_rank)]
            total = total + lax.ppermute(value, "rank", pairs)
        return total

    def gather_everyone(value):
        spread = jnp.broadcast_to(value[None], (n_all,) + value.shape)
        got = lax.all_to_all(spread, everyone, 0, 0)
        return got.reshape(n_rows, n_rank, value.shape[-1])

    def per_device(left_factor, right_factor, left_plan, right_plan, log_inner, left_mass, right_mass):
        precise = lax.Precision.HIGHEST
        columns = left_plan.shape[0]
        depth = left_factor.shape[0]
        mine = lax.axis_index("rank")
        left_round = left_plan.astype(jnp.bfloat16)
        right_round = right_plan.astype(jnp.bfloat16)
        masses = jnp.stack([jnp.sum(left_mass), jnp.sum(right_mass)])
        masses = jnp.broadcast_to(masses[:, None], (2, columns))
        masses = jnp.concatenate([masses, jnp.zeros((6, columns), jnp.float32)])
        sums = sum_over_rows(
            jnp.concatenate(
                [
                    contract_points(right_factor, right_round),
                    contract_points(left_factor, left_round),
                    masses,
                ]
            )
        )
        proj_right = sums[:depth]
        proj_left = sums[depth : 2 * depth]
        total_left = sums[2 * depth, 0]
        total_right = sums[2 * depth + 1, 0]
        inner_mass = total_left / RANK * jnp.exp(log_inner)
        scaled_right = (proj_right / inner_mass[None, :]).astype(jnp.bfloat16)
        scaled_left = (proj_left / inner_mass[None, :]).astype(jnp.bfloat16)
        grad_left = expand_points(scaled_right, left_factor)
        grad_right = expand_points(scaled_left, right_factor)
        pairing = jnp.sum(scaled_right.astype(jnp.float32) * proj_left, axis=0)
        grad_inner = -pairing / inner_mass
        local_top = jnp.maximum(
            jnp.maximum(jnp.max(jnp.abs(grad_left)), jnp.max(jnp.abs(grad_right))),
            jnp.max(jnp.abs(grad_inner)),
        )
        largest = jnp.max(gather_everyone(jnp.full((1, 128), local_top)))
        step_size = 5.0 / jnp.maximum(largest, 0.25)
        tilted_left = left_plan * jnp.exp(-step_size * grad_left)
        tilted_right = right_plan * jnp.exp(-step_size * grad_right)
        inner_mass = inner_mass * jnp.exp(-step_size * grad_inner)
        right_norm = right_mass * (total_left / total_right)
        row_scale_left = left_mass
        row_scale_right = right_norm
        own_left = jnp.ones((columns,), jnp.float32)
        own_right = jnp.ones((columns,), jnp.float32)
        own_inner = inner_mass
        for repeat in range(ITERS):
            rows_both = sum_over_rank(
                jnp.stack(
                    [
                        jnp.dot(own_left, tilted_left, precision=precise),
                        jnp.dot(own_right, tilted_right, precision=precise),
                    ]
                )
            )
            row_scale_left = left_mass / rows_both[0]
            row_scale_right = right_norm / rows_both[1]
            partial = jnp.concatenate(
                [
                    jnp.dot(tilted_left, row_scale_left, precision=precise),
                    jnp.dot(tilted_right, row_scale_right, precision=precise),
                ]
            )
            parts = gather_everyone(partial[None])
            total = jnp.sum(lax.dynamic_index_in_dim(parts, mine, 1, False), axis=0)
            own_inner, own_left, own_right = balance(
                own_inner, own_left, total[:columns], own_right, total[columns:]
            )
        new_left = row_scale_left[None, :] * tilted_left * own_left[:, None]
        new_right = row_scale_right[None, :] * tilted_right * own_right[:, None]
        new_log_inner = jnp.log(own_inner) - jnp.log(total_left / RANK)
        return (new_left, new_right, new_log_inner)

    in_specs = (
        P(None, "rows"),
        P(None, "rows"),
        P("rank", "rows"),
        P("rank", "rows"),
        P("rank"),
        P("rows"),
        P("rows"),
    )
    out_specs = (P("rank", "rows"), P("rank", "rows"), P("rank"))
    return jax.shard_map(
        per_device, mesh=mesh, in_specs=in_specs, out_specs=out_specs, check_vma=False
    )
```

```python
import functools

import jax
import jax.numpy as jnp
from jax import lax
from jax.experimental import pallas as pl
from jax.experimental.pallas import tpu as pltpu
from jax.sharding import PartitionSpec as P

RANK = 256
ITERS = 3
LANES = 128


def dot(a, b, a_dim, b_dim):
    return lax.dot_general(
        a, b, (((a_dim,), (b_dim,)), ((), ())), preferred_element_type=jnp.float32
    )


def call(body, out_shape, *args):
    specs = [pl.BlockSpec(memory_space=pltpu.SMEM)]
    specs += [pl.BlockSpec(memory_space=pltpu.VMEM) for _ in args[1:]]
    outs = jax.tree.map(lambda _: pl.BlockSpec(memory_space=pltpu.VMEM), out_shape)
    return pl.pallas_call(
        body,
        out_shape=out_shape,
        in_specs=specs,
        out_specs=outs,
        compiler_params=pltpu.CompilerParams(vmem_limit_bytes=32 * 2**20),
    )(*args)


def f32(*shape):
    return jax.ShapeDtypeStruct(shape, jnp.float32)


def project(n_rank, at, left_factor, right_factor, left_plan, right_plan, left_mass, right_mass, sums, *blocks):
    depth = left_factor.shape[0]
    columns = left_plan.shape[0]
    span = left_plan.shape[1] // n_rank
    sums[:depth, :columns] = dot(right_factor[...], right_plan[...].astype(jnp.bfloat16), 1, 1)
    sums[:depth, columns:] = dot(left_factor[...], left_plan[...].astype(jnp.bfloat16), 1, 1)
    sums[depth:, :columns] = jnp.full((8, columns), jnp.sum(left_mass[...]))
    sums[depth:, columns:] = jnp.full((8, columns), jnp.sum(right_mass[...]))
    for shift in range(n_rank):
        start = pl.multiple_of(((at[0] + shift) % n_rank) * span, LANES)
        blocks[shift][0] = left_plan[:, pl.ds(start, span)]
        blocks[shift][1] = right_plan[:, pl.ds(start, span)]


def gradients(at, sums, log_inner, left_factor, right_factor, scaled, grad_left, grad_right, top):
    depth = left_factor.shape[0]
    columns = log_inner.shape[1]
    total_left = sums[depth : depth + 1, :columns]
    inner = total_left / RANK * jnp.exp(log_inner[...])
    proj_left = sums[:depth, columns:]
    scaled_right = (sums[:depth, :columns] / inner).astype(jnp.bfloat16)
    scaled_left = (proj_left / inner).astype(jnp.bfloat16)
    up = dot(scaled_right, left_factor[...], 0, 0)
    grad_left[...] = up
    peak = jnp.max(jnp.abs(up))
    up = dot(scaled_left, right_factor[...], 0, 0)
    grad_right[...] = up
    peak = jnp.maximum(peak, jnp.max(jnp.abs(up)))
    right = scaled_right.astype(jnp.float32)
    pairing = jnp.sum(right * proj_left, axis=0, keepdims=True)
    grad_inner = -pairing / inner
    peak = jnp.maximum(peak, jnp.max(jnp.abs(grad_inner)))
    scaled[:depth, :columns] = right
    scaled[:depth, columns:] = scaled_left.astype(jnp.float32)
    scaled[depth:, :columns] = jnp.broadcast_to(inner, (8, columns))
    scaled[depth:, columns:] = jnp.broadcast_to(grad_inner, (8, columns))
    top[...] = jnp.full((1, LANES), peak)


def as_column(row):
    return jnp.broadcast_to(row, (LANES, row.shape[1])).T


def turn(n_rank, at, left_factor, right_factor, left_mass, right_mass, sums, *refs):
    scaled = refs[:n_rank]
    plans = refs[n_rank : 2 * n_rank]
    plan_out, grad_out, mass_out, inner_out = refs[2 * n_rank :]
    depth = left_factor.shape[0]
    columns = sums.shape[1] // 2
    span = left_factor.shape[1] // n_rank
    start = pl.multiple_of(at[0] * span, LANES)
    here = pl.ds(start, span)
    right = jnp.concatenate([s[:depth, :columns] for s in scaled], axis=1)
    left = jnp.concatenate([s[:depth, columns:] for s in scaled], axis=1)
    grad_out[0] = dot(left_factor[:, here], right.astype(jnp.bfloat16), 0, 0)
    grad_out[1] = dot(right_factor[:, here], left.astype(jnp.bfloat16), 0, 0)
    for side in range(2):
        plan_out[side] = jnp.concatenate([p[side].T for p in plans], axis=1)
    ratio = sums[depth : depth + 1, :1] / sums[depth : depth + 1, columns : columns + 1]
    mass_out[0] = as_column(left_mass[:, here])
    mass_out[1] = as_column(right_mass[:, here] * ratio)
    inner = jnp.concatenate([s[depth : depth + 1, :columns] for s in scaled], axis=1)
    grad_inner = jnp.concatenate([s[depth : depth + 1, columns:] for s in scaled], axis=1)
    inner_out[0:1] = inner
    inner_out[1:2] = grad_inner


def rolled(pair, shift):
    rows = jnp.concatenate([pair[0], pair[1]] * 4, axis=0)
    return pltpu.roll(rows, shift, 1)


def totals(n_rank, at, side_sum, all_k, columns):
    both = jnp.sum(side_sum[...], axis=0)
    half = all_k // LANES
    left = jnp.concatenate([both[i : i + 1] for i in range(half)], axis=1)
    right = jnp.concatenate([both[half + i : half + i + 1] for i in range(half)], axis=1)
    moved = rolled((left, right), ((n_rank - at[0]) % n_rank) * columns)
    return moved[0:1], moved[1:2]


def sweep(n_rank, at, columns, tilted, mass, scales, part, rows=None):
    got = []
    for side in range(2):
        block = tilted[side]
        weighted = block if scales is None else block * scales[side]
        row = mass[side] / jnp.sum(weighted, axis=1, keepdims=True)
        if rows is not None:
            rows[side] = row
        got.append(jnp.sum(block * row[:, :1], axis=0, keepdims=True))
    moved = rolled(got, at[0] * columns)
    half = moved.shape[1] // LANES
    for side in range(2):
        for i in range(half):
            part[side * half + i : side * half + i + 1] = moved[side : side + 1, i * LANES : (i + 1) * LANES]


def balance(inner, scales, sums):
    mixed = jnp.log(inner) + jnp.log(scales[0] * sums[0]) + jnp.log(scales[1] * sums[1])
    inner = jnp.exp(mixed / 3.0)
    return inner, (inner / sums[0], inner / sums[1])


def step_of(tops):
    return 5.0 / jnp.maximum(jnp.max(tops[...]), 0.25)


def tilt(n_rank, columns, at, tops, plan, grad, mass, inner_in, tilted, inner_out, part):
    step = step_of(tops)
    for side in range(2):
        tilted[side] = plan[side] * jnp.exp(-step * grad[side])
    inner_out[0:1] = inner_in[0:1] * jnp.exp(-step * inner_in[1:2])
    sweep(n_rank, at, columns, tilted, mass, None, part)


def again(n_rank, columns, first, at, parts, tilted, mass, state_in, state_out, part, rows):
    all_k = tilted.shape[2]
    sums = totals(n_rank, at, parts, all_k, columns)
    ones = jnp.ones((1, all_k), jnp.float32)
    old = (ones, ones) if first else (state_in[1:2], state_in[2:3])
    inner, scales = balance(state_in[0:1], old, sums)
    state_out[0:1] = inner
    state_out[1:2] = scales[0]
    state_out[2:3] = scales[1]
    sweep(n_rank, at, columns, tilted, mass, scales, part, rows)


def lay_rows(at, rows, flat):
    for side in range(2):
        flat[side : side + 1] = rows[side].T[0:1]


def own_points(n_rank, at, tops, left_plan, right_plan, grad_left, grad_right, *refs):
    flats = refs[:n_rank]
    left, right = refs[n_rank:]
    step = step_of(tops)
    span = left_plan.shape[1] // n_rank
    for shift in range(n_rank):
        start = pl.multiple_of(((at[0] + shift) % n_rank) * span, LANES)
        here = pl.ds(start, span)
        row = flats[shift]
        left[:, here] = row[0:1] * (left_plan[:, here] * jnp.exp(-step * grad_left[:, here]))
        right[:, here] = row[1:2] * (right_plan[:, here] * jnp.exp(-step * grad_right[:, here]))


def finish(n_rank, columns, at, parts, state, sums, left, right, new_left, new_right, new_log):
    all_k = state.shape[1]
    got = totals(n_rank, at, parts, all_k, columns)
    inner, scales = balance(state[0:1], (state[1:2], state[2:3]), got)
    depth = sums.shape[0] - 8
    new_log[...] = jnp.log(inner[:, :columns]) - jnp.log(sums[depth : depth + 1, :columns] / RANK)
    new_left[...] = left[...] * as_column(scales[0])[:columns, :1]
    new_right[...] = right[...] * as_column(scales[1])[:columns, :1]


def solution(mesh):
    n_rows = mesh.shape["rows"]
    n_rank = mesh.shape["rank"]
    everyone = ("rows", "rank")
    n_all = n_rows * n_rank

    def sum_over_rows(value):
        if n_rows & (n_rows - 1):
            return lax.psum(value, "rows")
        stride = 1
        while stride < n_rows:
            pairs = [(i, i ^ stride) for i in range(n_rows)]
            value = value + lax.ppermute(value, "rows", pairs)
            stride *= 2
        return value

    def to_everyone(value):
        spread = jnp.broadcast_to(value[None], (n_all,) + value.shape)
        return lax.all_to_all(spread, everyone, 0, 0)

    def from_rank(value, shift):
        return lax.ppermute(value, "rank", [((i + shift) % n_rank, i) for i in range(n_rank)])

    def per_device(left_factor, right_factor, left_plan, right_plan, log_inner, left_mass, right_mass):
        depth, points = left_factor.shape
        columns = left_plan.shape[0]
        all_k = columns * n_rank
        span = points // n_rank
        at = lax.axis_index("rank").reshape(1)
        left_mass = left_mass.reshape(1, points)
        right_mass = right_mass.reshape(1, points)

        sums, *blocks = call(
            functools.partial(project, n_rank),
            [f32(depth + 8, 2 * columns)] + [f32(2, columns, span)] * n_rank,
            at, left_factor, right_factor, left_plan, right_plan, left_mass, right_mass,
        )
        plans = [blocks[0]]
        for shift in range(1, n_rank):
            plans.append(
                lax.ppermute(blocks[shift], "rank", [(i, (i + shift) % n_rank) for i in range(n_rank)])
            )
        plans = [plans[(n_rank - s) % n_rank] for s in range(n_rank)]
        sums = sum_over_rows(sums)
        scaled, grad_left, grad_right, top = call(
            gradients,
            [f32(depth + 8, 2 * columns), f32(columns, points), f32(columns, points), f32(1, LANES)],
            at, sums, log_inner.reshape(1, columns), left_factor, right_factor,
        )
        tops = to_everyone(top)
        scaleds = [scaled] + [from_rank(scaled, s) for s in range(1, n_rank)]
        plan, grad, mass, inner = call(
            functools.partial(turn, n_rank),
            [f32(2, span, all_k), f32(2, span, all_k), f32(2, span, LANES), f32(8, all_k)],
            at, left_factor, right_factor, left_mass, right_mass, sums, *scaleds, *plans,
        )
        part_shape = f32(2 * all_k // LANES, LANES)
        tilted, state, part = call(
            functools.partial(tilt, n_rank, columns),
            [f32(2, span, all_k), f32(8, all_k), part_shape],
            at, tops, plan, grad, mass, inner,
        )
        for repeat in range(1, ITERS):
            parts = to_everyone(part)
            state, part, rows = call(
                functools.partial(again, n_rank, columns, repeat == 1),
                [f32(8, all_k), part_shape, f32(2, span, LANES)],
                at, parts, tilted, mass, state,
            )
        parts = to_everyone(part)
        flat = call(lay_rows, f32(2, span), at, rows)
        flats = [flat] + [from_rank(flat, s) for s in range(1, n_rank)]
        left, right = call(
            functools.partial(own_points, n_rank),
            [f32(columns, points)] * 2,
            at, tops, left_plan, right_plan, grad_left, grad_right, *flats,
        )
        new_left, new_right, new_log = call(
            functools.partial(finish, n_rank, columns),
            [f32(columns, points), f32(columns, points), f32(1, columns)],
            at, parts, state, sums, left, right,
        )
        return (new_left, new_right, new_log.reshape(columns))

    in_specs = (
        P(None, "rows"),
        P(None, "rows"),
        P("rank", "rows"),
        P("rank", "rows"),
        P("rank"),
        P("rows"),
        P("rows"),
    )
    out_specs = (P("rank", "rows"), P("rank", "rows"), P("rank"))
    return jax.shard_map(
        per_device, mesh=mesh, in_specs=in_specs, out_specs=out_specs, check_vma=False
    )
```

```python
import functools

import jax
import jax.numpy as jnp
from jax import lax
from jax.experimental import pallas as pl
from jax.experimental.pallas import tpu as pltpu
from jax.sharding import PartitionSpec as P

RANK = 256
ITERS = 3
LANES = 128


def dot(a, b, a_dim, b_dim):
    return lax.dot_general(
        a, b, (((a_dim,), (b_dim,)), ((), ())), preferred_element_type=jnp.float32
    )


HBM = pl.BlockSpec(memory_space=pltpu.HBM)
VMEM = pl.BlockSpec(memory_space=pltpu.VMEM)


def call(body, outs, args, scratch=(), aliases=None):
    specs = [pl.BlockSpec(memory_space=pltpu.SMEM)]
    specs += [spec for _, spec in args[1:]]
    return pl.pallas_call(
        body,
        out_shape=[shape for shape, _ in outs],
        in_specs=specs,
        out_specs=[spec for _, spec in outs],
        scratch_shapes=list(scratch),
        input_output_aliases=aliases or {},
        compiler_params=pltpu.CompilerParams(vmem_limit_bytes=16 * 2**20),
    )(args[0], *[array for array, _ in args[1:]])


def on_chip(*arrays):
    return [(array, VMEM) for array in arrays]


def anywhere(*arrays):
    return [(array, pl.BlockSpec(memory_space=pl.ANY)) for array in arrays]


def in_hbm(*arrays):
    pinned = [
        array if isinstance(array, jax.ShapeDtypeStruct) else pltpu.with_memory_space_constraint(array, pltpu.HBM)
        for array in arrays
    ]
    return [(array, HBM) for array in pinned]


def f32(*shape):
    return jax.ShapeDtypeStruct(shape, jnp.float32)


def project(n_rank, at, left_factor, right_factor, left_plan, right_plan, left_mass, right_mass, log_inner, *refs):
    sums, left_kept, right_kept, log_kept = refs[:4]
    blocks = refs[4 : 4 + n_rank]
    masses, done = refs[4 + n_rank :]
    depth = left_factor.shape[0]
    columns = left_plan.shape[0]
    span = left_plan.shape[1] // n_rank
    starts = [pl.multiple_of(((at[0] + shift) % n_rank) * span, LANES) for shift in range(n_rank)]
    pairs = [(right_factor, right_kept), (left_factor, left_kept)]
    for side, plan in ((1, right_plan), (0, left_plan)):
        for shift in range(n_rank):
            pairs.append((plan.at[:, pl.ds(starts[shift], span)], blocks[shift].at[side]))
    pairs += [
        (left_mass, masses.at[0:1]),
        (right_mass, masses.at[1:2]),
        (log_inner, log_kept),
    ]
    copies = [pltpu.make_async_copy(src, dst, done.at[i]) for i, (src, dst) in enumerate(pairs)]
    for copy in copies:
        copy.start()
    for side, kept in ((1, right_kept), (0, left_kept)):
        copies[1 - side].wait()
        total = jnp.zeros((depth, columns), jnp.float32)
        for shift in range(n_rank):
            copies[2 + (1 - side) * n_rank + shift].wait()
            here = kept[:, pl.ds(starts[shift], span)]
            total = total + dot(here, blocks[shift][side].astype(jnp.bfloat16), 1, 1)
        place = slice(0, columns) if side else slice(columns, 2 * columns)
        sums[:depth, place] = total
    for copy in copies[2 + 2 * n_rank :]:
        copy.wait()
    sums[depth:, :columns] = jnp.full((8, columns), jnp.sum(masses[0:1]))
    sums[depth:, columns:] = jnp.full((8, columns), jnp.sum(masses[1:2]))


def gradients(at, sums, log_inner, left_factor, right_factor, scaled, top):
    depth = left_factor.shape[0]
    columns = log_inner.shape[1]
    total_left = sums[depth : depth + 1, :columns]
    inner = total_left / RANK * jnp.exp(log_inner[...])
    proj_left = sums[:depth, columns:]
    scaled_right = (sums[:depth, :columns] / inner).astype(jnp.bfloat16)
    scaled_left = (proj_left / inner).astype(jnp.bfloat16)
    right = scaled_right.astype(jnp.float32)
    scaled[:depth, :columns] = right
    scaled[:depth, columns:] = scaled_left.astype(jnp.float32)
    pairing = jnp.sum(right * proj_left, axis=0, keepdims=True)
    grad_inner = -pairing / inner
    scaled[depth:, :columns] = jnp.broadcast_to(inner, (8, columns))
    scaled[depth:, columns:] = jnp.broadcast_to(grad_inner, (8, columns))
    peak = jnp.max(jnp.abs(grad_inner))
    peak = jnp.maximum(peak, jnp.max(jnp.abs(dot(scaled_right, left_factor[...], 0, 0))))
    peak = jnp.maximum(peak, jnp.max(jnp.abs(dot(scaled_left, right_factor[...], 0, 0))))
    top[...] = jnp.full(top.shape, peak)


def as_column(row):
    return jnp.broadcast_to(row, (LANES, row.shape[1])).T


def turn(n_rank, at, sums, left_factor, right_factor, left_mass, right_mass, *refs):
    scaled_in = refs[:n_rank]
    plans_in = refs[n_rank : 2 * n_rank]
    plan_out, grad_out, mass_out, inner_out, factors, masses, scaled, plans, done = refs[2 * n_rank :]
    depth = left_factor.shape[0]
    columns = sums.shape[1] // 2
    span = left_factor.shape[1] // n_rank
    here = pl.ds(pl.multiple_of(at[0] * span, LANES), span)
    pairs = [(plans_in[s], plans.at[s]) for s in range(n_rank)]
    pairs += [(left_mass.at[:, here], masses.at[0]), (right_mass.at[:, here], masses.at[1])]
    early = len(pairs)
    pairs += [(left_factor.at[:, here], factors.at[0]), (right_factor.at[:, here], factors.at[1])]
    pairs += [(scaled_in[s], scaled.at[s]) for s in range(n_rank)]
    copies = [pltpu.make_async_copy(src, dst, done.at[i]) for i, (src, dst) in enumerate(pairs)]
    for copy in copies:
        copy.start()
    for copy in copies[:early]:
        copy.wait()
    for side in range(2):
        plan_out[side] = jnp.concatenate([plans[s, side].T for s in range(n_rank)], axis=1)
    ratio = sums[depth : depth + 1, :1] / sums[depth : depth + 1, columns : columns + 1]
    mass_out[0] = as_column(masses[0])
    mass_out[1] = as_column(masses[1] * ratio)
    for copy in copies[early:]:
        copy.wait()
    right = jnp.concatenate([scaled[s, :depth, :columns] for s in range(n_rank)], axis=1)
    left = jnp.concatenate([scaled[s, :depth, columns:] for s in range(n_rank)], axis=1)
    grad_out[0] = dot(factors[0], right.astype(jnp.bfloat16), 0, 0)
    grad_out[1] = dot(factors[1], left.astype(jnp.bfloat16), 0, 0)
    for row, place in ((0, slice(0, columns)), (1, slice(columns, 2 * columns))):
        parts = [scaled[s, depth : depth + 1, place] for s in range(n_rank)]
        inner_out[row : row + 1] = jnp.concatenate(parts, axis=1)


def rolled(pair, shift):
    rows = jnp.concatenate([pair[0], pair[1]] * 4, axis=0)
    return pltpu.roll(rows, shift, 1)


def totals(n_rank, at, side_sum, all_k, columns):
    both = jnp.sum(side_sum[...], axis=0)
    half = all_k // LANES
    left = jnp.concatenate([both[i : i + 1] for i in range(half)], axis=1)
    right = jnp.concatenate([both[half + i : half + i + 1] for i in range(half)], axis=1)
    moved = rolled((left, right), ((n_rank - at[0]) % n_rank) * columns)
    return moved[0:1], moved[1:2]


def sweep(n_rank, at, columns, tilted, mass, scales, part, rows=None):
    got = []
    for side in range(2):
        block = tilted[side]
        weighted = block if scales is None else block * scales[side]
        row = mass[side] / jnp.sum(weighted, axis=1, keepdims=True)
        if rows is not None:
            rows[side] = row
        got.append(jnp.sum(block * row[:, :1], axis=0, keepdims=True))
    moved = rolled(got, at[0] * columns)
    half = moved.shape[1] // LANES
    pieces = [
        moved[side : side + 1, i * LANES : (i + 1) * LANES] for side in range(2) for i in range(half)
    ]
    part[...] = jnp.broadcast_to(jnp.concatenate(pieces, axis=0)[None], part.shape)


def balance(inner, scales, sums):
    mixed = jnp.log(inner) + jnp.log(scales[0] * sums[0]) + jnp.log(scales[1] * sums[1])
    inner = jnp.exp(mixed / 3.0)
    return inner, (inner / sums[0], inner / sums[1])


def step_of(tops):
    return 5.0 / jnp.maximum(jnp.max(tops[...]), 0.25)


def tilt(n_rank, columns, at, tops, plan, grad, mass, inner_in, tilted, inner_out, part):
    step = step_of(tops)
    for side in range(2):
        tilted[side] = plan[side] * jnp.exp(-step * grad[side])
    inner_out[0:1] = inner_in[0:1] * jnp.exp(-step * inner_in[1:2])
    sweep(n_rank, at, columns, tilted, mass, None, part)


def again(n_rank, columns, first, at, parts, tilted, mass, state_in, state_out, part, rows=None):
    all_k = tilted.shape[2]
    sums = totals(n_rank, at, parts, all_k, columns)
    ones = jnp.ones((1, all_k), jnp.float32)
    old = (ones, ones) if first else (state_in[1:2], state_in[2:3])
    inner, scales = balance(state_in[0:1], old, sums)
    state_out[0:1] = inner
    state_out[1:2] = scales[0]
    state_out[2:3] = scales[1]
    sweep(n_rank, at, columns, tilted, mass, scales, part, rows)


def lay_rows(at, rows, flat):
    for side in range(2):
        flat[side : side + 1] = rows[side].T[0:1]


def own_points(n_rank, at, tops, scaled, left_factor, right_factor, left_plan, right_plan, *refs):
    flats = refs[:n_rank]
    left, right, left_in, right_in, left_was, right_was, done = refs[n_rank:]
    pairs = [
        (left_factor, left_in),
        (right_factor, right_in),
        (left_plan, left_was),
        (right_plan, right_was),
    ]
    copies = [pltpu.make_async_copy(src, dst, done.at[i]) for i, (src, dst) in enumerate(pairs)]
    for copy in copies:
        copy.start()
    step = step_of(tops)
    depth = left_factor.shape[0]
    columns, points = left_plan.shape
    span = points // n_rank
    scaled_right = scaled[:depth, :columns].astype(jnp.bfloat16)
    scaled_left = scaled[:depth, columns:].astype(jnp.bfloat16)
    for copy in copies:
        copy.wait()
    for shift in range(n_rank):
        start = pl.multiple_of(((at[0] + shift) % n_rank) * span, LANES)
        here = pl.ds(start, span)
        row = flats[shift]
        up = dot(scaled_right, left_in[:, here], 0, 0)
        left[:, here] = row[0:1] * (left_was[:, here] * jnp.exp(-step * up))
        up = dot(scaled_left, right_in[:, here], 0, 0)
        right[:, here] = row[1:2] * (right_was[:, here] * jnp.exp(-step * up))


def finish(n_rank, columns, at, parts, state, sums, left, right, new_left, new_right, new_log, left_out, right_out, done):
    all_k = state.shape[1]
    got = totals(n_rank, at, parts, all_k, columns)
    inner, scales = balance(state[0:1], (state[1:2], state[2:3]), got)
    depth = sums.shape[0] - 8
    copies = []
    for side, (was, out, new) in enumerate(((left, left_out, new_left), (right, right_out, new_right))):
        out[...] = was[...] * as_column(scales[side])[:columns, :1]
        copies.append(pltpu.make_async_copy(out, new, done.at[side]))
        copies[-1].start()
    new_log[...] = jnp.log(inner[:, :columns]) - jnp.log(sums[depth : depth + 1, :columns] / RANK)
    for copy in copies:
        copy.wait()


def solution(mesh):
    n_rows = mesh.shape["rows"]
    n_rank = mesh.shape["rank"]
    everyone = ("rows", "rank")
    n_all = n_rows * n_rank

    def sum_over_rows(value):
        if n_rows & (n_rows - 1):
            return lax.psum(value, "rows")
        stride = 1
        while stride < n_rows:
            pairs = [(i, i ^ stride) for i in range(n_rows)]
            value = value + lax.ppermute(value, "rows", pairs)
            stride *= 2
        return value

    def to_everyone(value):
        return lax.all_to_all(value, everyone, 0, 0)

    def from_rank(value, shift):
        return lax.ppermute(value, "rank", [((i + shift) % n_rank, i) for i in range(n_rank)])

    def per_device(left_factor, right_factor, left_plan, right_plan, log_inner, left_mass, right_mass):
        depth, points = left_factor.shape
        columns = left_plan.shape[0]
        all_k = columns * n_rank
        span = points // n_rank
        at = lax.axis_index("rank").reshape(1)
        arguments = (
            left_factor, right_factor, left_plan, right_plan,
            left_mass.reshape(1, points), right_mass.reshape(1, points), log_inner.reshape(1, columns),
        )
        factor_shape = jax.ShapeDtypeStruct((depth, points), jnp.bfloat16)
        sums_shape = f32(depth + 8, 2 * columns)
        sums, left_kept, right_kept, log_kept, *blocks = call(
            functools.partial(project, n_rank),
            on_chip(sums_shape, factor_shape, factor_shape, f32(1, columns))
            + on_chip(*[f32(2, columns, span)] * n_rank),
            [at, *in_hbm(*arguments)],
            [pltpu.VMEM((2, points), jnp.float32), pltpu.SemaphoreType.DMA((5 + 2 * n_rank,))],
        )
        plans = [blocks[0]]
        for shift in range(1, n_rank):
            plans.append(
                lax.ppermute(blocks[shift], "rank", [(i, (i + shift) % n_rank) for i in range(n_rank)])
            )
        plans = [plans[(n_rank - s) % n_rank] for s in range(n_rank)]
        sums = sum_over_rows(sums)
        scaled, top = call(
            gradients,
            on_chip(sums_shape, f32(n_all, 1, LANES)),
            [at, *on_chip(sums, log_kept, left_kept, right_kept)],
        )
        tops = to_everyone(top)
        scaleds = [scaled] + [from_rank(scaled, s) for s in range(1, n_rank)]
        plan, grad, mass, inner = call(
            functools.partial(turn, n_rank),
            on_chip(f32(2, span, all_k), f32(2, span, all_k), f32(2, span, LANES), f32(8, all_k)),
            [at, *on_chip(sums), *in_hbm(*arguments[:2], *arguments[4:6]), *anywhere(*scaleds, *plans)],
            [
                pltpu.VMEM((2, depth, span), jnp.bfloat16),
                pltpu.VMEM((2, 1, span), jnp.float32),
                pltpu.VMEM((n_rank, depth + 8, 2 * columns), jnp.float32),
                pltpu.VMEM((n_rank, 2, columns, span), jnp.float32),
                pltpu.SemaphoreType.DMA((4 + 2 * n_rank,)),
            ],
        )
        part_shape = f32(n_all, 2 * all_k // LANES, LANES)
        tilted, state, part = call(
            functools.partial(tilt, n_rank, columns),
            on_chip(f32(2, span, all_k), f32(8, all_k), part_shape),
            [at, *on_chip(tops, plan, grad, mass, inner)],
            aliases={2: 0},
        )
        for repeat in range(1, ITERS):
            last = repeat == ITERS - 1
            parts = to_everyone(part)
            state, part, *rows = call(
                functools.partial(again, n_rank, columns, repeat == 1),
                on_chip(f32(8, all_k), part_shape, *[f32(2, span, LANES)] * last),
                [at, *on_chip(parts, tilted, mass, state)],
            )
        parts = to_everyone(part)
        (flat,) = call(lay_rows, on_chip(f32(2, span)), [at, *on_chip(*rows)])
        flats = [flat] + [from_rank(flat, s) for s in range(1, n_rank)]
        left, right = call(
            functools.partial(own_points, n_rank),
            on_chip(f32(columns, points), f32(columns, points)),
            [at, *on_chip(tops, scaled), *in_hbm(left_factor, right_factor, left_plan, right_plan), *on_chip(*flats)],
            [pltpu.VMEM((depth, points), jnp.bfloat16)] * 2
            + [pltpu.VMEM((columns, points), jnp.float32)] * 2
            + [pltpu.SemaphoreType.DMA((4,))],
        )
        new_left, new_right, new_log = call(
            functools.partial(finish, n_rank, columns),
            [*in_hbm(f32(columns, points), f32(columns, points)), *on_chip(f32(1, columns))],
            [at, *on_chip(parts, state, sums, left, right)],
            [pltpu.VMEM((columns, points), jnp.float32)] * 2 + [pltpu.SemaphoreType.DMA((2,))],
        )
        return (new_left, new_right, new_log.reshape(columns))

    in_specs = (
        P(None, "rows"),
        P(None, "rows"),
        P("rank", "rows"),
        P("rank", "rows"),
        P("rank"),
        P("rows"),
        P("rows"),
    )
    out_specs = (P("rank", "rows"), P("rank", "rows"), P("rank"))
    return jax.shard_map(
        per_device, mesh=mesh, in_specs=in_specs, out_specs=out_specs, check_vma=False
    )
```
